32 devices in a mesh: seq: 8 (over z, x), tp: 4 (over y, core).
Axes of the slice: x: 2, y: 2, z: 4, core: 2. Of those that a mesh axis runs over, the one named last changes fastest.
Arguments:
- packed_input: int32 [512, 5120], P('seq', 'tp'), may hold values from -2147483648 to 2147483646
- block_exponent: int32 [40, 4096], P('tp', 'seq'), may hold values from -5 to -1
- gate_input: bfloat16 [4096, 5120], P('seq', 'tp'), may hold values from -80 to 80
- state_write: bfloat16 [4096, 128], P('seq'), may hold values from -6 to 6
- state_read: bfloat16 [4096, 128], P('seq'), may hold values from -6 to 6
- log_decay: float32 [80, 4096], P('tp', 'seq'), may hold values from -1.6 to 0
- skip_weight: float32 [80], P('tp'), may hold values from 0.3 to 3
- norm_gain: float32 [5120], P('tp'), may hold values from 0.5 to 1.5
- out_weight: bfloat16 [5120, 2560], P('tp'), may hold values from -0.078125 to 0.078125
- out_cotangent: bfloat16 [4096, 2560], P('seq', 'tp'), may hold values from -6 to 6
Outputs:
- grad_input: bfloat16 [4096, 5120], P('seq', 'tp')
- grad_gate: bfloat16 [4096, 5120], P('seq', 'tp')
- grad_write: float32 [4096, 128], P('seq')
- grad_read: float32 [4096, 128], P('seq')
- grad_decay: float32 [80, 4096], P('tp', 'seq')
- grad_skip: float32 [80], P('tp')
- grad_gain: float32 [5120], P('tp')
- grad_out_weight: float32 [5120, 2560], P('tp', 'seq')
The draws below stay inside these ranges and needn't reach their ends.
All inputs are finite; a program needn't handle non-finite values.
Results may differ from the reference program's by a relative error of at most 0.0049.
Values may be sent and summed in bfloat16 or wider, within the bound.
A program may use at most 128 MiB of HBM per device.

```python
import math
import jax
import jax.numpy as jnp
from jax import lax

D = 2560
HEAD_NUMBER = 80
N = 128
QBLOCK = 128
TOK_DEV = 512
TOKEN_NUMBER = 4096
HP = 5120


def draw_gate_input(key, part):
    first_key, second_key = jax.random.split(jax.random.fold_in(key, 11))
    column_pos = jnp.arange(HP, dtype=jnp.float32) / (HP - 1)
    base = jax.random.truncated_normal(first_key, -4.0, 4.0, (TOKEN_NUMBER, HP), jnp.float32)
    column_scale = 3.0 ** column_pos
    row_scale = jnp.exp(jax.random.uniform(second_key, (TOKEN_NUMBER, 1), jnp.float32, math.log(0.3), math.log(3.0)))
    return (base * column_scale[None, :] * row_scale).astype(jnp.bfloat16)


def draw_log_decay(key, part):
    random_keys = jax.random.split(jax.random.fold_in(key, 23), 7)
    slow_share = 0.5
    is_slow = jax.random.uniform(random_keys[0], (HEAD_NUMBER, 1), jnp.float32) < slow_share
    slow_rate = jax.random.uniform(random_keys[1], (HEAD_NUMBER, 1), jnp.float32, 0.15, 0.6) / TOKEN_NUMBER
    fast_rate = jnp.exp(jax.random.uniform(random_keys[2], (HEAD_NUMBER, 1), jnp.float32, math.log(1.0 / 50.0), math.log(1.0 / 30.0)))
    baseline_rate = jnp.where(is_slow, slow_rate, fast_rate)
    coarse_values = jnp.exp(jax.random.uniform(random_keys[3], (HEAD_NUMBER, TOKEN_NUMBER), jnp.float32, math.log(0.5), math.log(2.0)))
    block_multiplier = jnp.exp(jax.random.uniform(random_keys[4], (HEAD_NUMBER, TOKEN_NUMBER // TOK_DEV), jnp.float32, math.log(0.5), math.log(2.0)))
    block_multiplier = jnp.repeat(block_multiplier, TOK_DEV, axis=1)
    spike_position = jax.random.randint(random_keys[5], (HEAD_NUMBER, 2), 0, TOKEN_NUMBER)
    spike_magnitude = jax.random.uniform(random_keys[6], (HEAD_NUMBER, 2), jnp.float32, 0.22, 0.69)
    token_places = jnp.arange(TOKEN_NUMBER)[None, :]
    spike_list = jnp.where(token_places == spike_position[:, 0:1], spike_magnitude[:, 0:1], 0.0) + jnp.where(token_places == spike_position[:, 1:2], spike_magnitude[:, 1:2], 0.0)
    return -(baseline_rate * coarse_values * block_multiplier + spike_list)


def set_ends(entries, rng, least, high):
    longest = entries.shape.index(max(entries.shape))
    spots = []
    for shift in (0, 1):
        where = [jax.random.randint(jax.random.fold_in(rng, axis), (), 0, length) for axis, length in enumerate(entries.shape)]
        where[longest] = (where[longest] + shift) % entries.shape[longest]
        spots.append(tuple(where))
    return entries.at[spots[0]].set(least).at[spots[1]].set(high)


def levels(rng, shape, cuts, low, high):
    gain = 1.0
    for axis_at, parts in cuts:
        steps = jax.random.uniform(jax.random.fold_in(jax.random.fold_in(rng, 6), axis_at), (parts,), jnp.float32, low / len(cuts), high / len(cuts))
        gain = gain * jnp.repeat(jnp.exp(steps), shape[axis_at] // parts).reshape((-1,) + (1,) * (len(shape) - 1 - axis_at))
    return gain


def bell_draw(stream_key, extent, scale, limit, pieces=(), kind=jnp.bfloat16):
    drawn = jax.random.normal(stream_key, extent, jnp.float32) * scale
    if len(pieces) > 0:
        drawn = levels(stream_key, extent, pieces, -0.22, 0.18) * drawn
    return jnp.clip(drawn, min=-limit, max=limit).astype(kind)


def setup_inputs(seed: int = 0) -> dict:
    splits = jax.random.split(jax.random.key(seed), 11)
    return {
        "packed_input": set_ends(jax.random.randint(splits[0], (TOKEN_NUMBER // 8, HP), -2147483648, 2147483647), jax.random.fold_in(splits[0], 1), -2147483648, 2147483646).astype(jnp.int32),
        "block_exponent": set_ends(jax.random.randint(splits[1], (HP // QBLOCK, TOKEN_NUMBER), -5, 0), jax.random.fold_in(splits[1], 1), -5, -1).astype(jnp.int32),
        "gate_input": draw_gate_input(jax.random.fold_in(splits[10], 71), 0),
        "state_write": bell_draw(splits[3], (TOKEN_NUMBER, N), 1.0, 6.0, ((0, 8),)),
        "state_read": bell_draw(splits[4], (TOKEN_NUMBER, N), 1.0, 6.0, ((0, 8),)),
        "log_decay": draw_log_decay(jax.random.fold_in(splits[10], 71), 0),
        "skip_weight": jnp.clip(jnp.exp(math.log(3.0) - 2.3025851 * jax.random.uniform(splits[6], (HEAD_NUMBER,), jnp.float32) ** levels(splits[6], (HEAD_NUMBER,), ((0, 4),), -0.2, 0.2)), 0.3, 3.0),
        "norm_gain": jnp.clip(1.0 + 0.1 * jax.random.normal(splits[7], (HP,), jnp.float32), 0.5, 1.5),
        "out_weight": bell_draw(splits[8], (HP, D), HP ** -0.5, 0.078125, ((0, 4),)),
        "out_cotangent": bell_draw(splits[9], (TOKEN_NUMBER, D), 1.0, 6.0, ((0, 8), (1, 4))),
    }


PRECISE = lax.Precision.HIGHEST

def dequantize(packed_words, exponents):
    shifts = 4 * jnp.arange(8, dtype=jnp.int32)
    fields = jnp.bitwise_and(jnp.right_shift(packed_words[:, None, :], shifts[None, :, None]), 15) - 8
    fields = fields.reshape(packed_words.shape[0] * 8, packed_words.shape[1])
    factors = jnp.exp2(exponents.astype(jnp.float32))
    group_width = fields.shape[1] // exponents.shape[0]
    factors = jnp.repeat(factors.T, group_width, axis=1)
    return (fields.astype(jnp.float32) * factors).astype(jnp.bfloat16)

def lower_decays(seg_sum):
    length = seg_sum.shape[1]
    is_lower = (jnp.arange(length)[:, None] >= jnp.arange(length)[None, :])[None]
    spread = seg_sum[:, :, None] - seg_sum[:, None, :]
    return jnp.where(is_lower, jnp.exp(jnp.where(is_lower, spread, 0.0)), 0.0)

def block_step(state_now, inputs):
    x_part, decay_part, write_part, read_part = inputs
    seg_sum = jnp.cumsum(decay_part, axis=1)
    mixing = lower_decays(seg_sum) * jnp.dot(read_part, write_part.T, precision=PRECISE)[None]
    carried_in = jnp.einsum('in,hpn->ihp', read_part, state_now, precision=PRECISE)
    result = jnp.einsum('hij,jhp->ihp', mixing, x_part, precision=PRECISE) + jnp.exp(seg_sum).T[:, :, None] * carried_in
    end_weight = jnp.exp(seg_sum[:, -1:] - seg_sum)
    state_next = jnp.exp(seg_sum[:, -1])[:, None, None] * state_now + jnp.einsum('jhp,jn->hpn', x_part * end_weight.T[:, :, None], write_part, precision=PRECISE)
    return (state_next, result)

def scan_states(x_heads, log_decay, write_rows, read_rows):
    total, head_count, head_width = x_heads.shape
    block_len = min(256, TOK_DEV)
    blocks = total // block_len
    x_blocks = x_heads.reshape(blocks, block_len, head_count, head_width)
    decay_blocks = log_decay.reshape(head_count, blocks, block_len).transpose(1, 0, 2)
    write_blocks = write_rows.reshape(blocks, block_len, -1)
    read_blocks = read_rows.reshape(blocks, block_len, -1)
    initial = jnp.zeros((head_count, head_width, write_rows.shape[1]), jnp.float32)
    _, outputs = lax.scan(jax.checkpoint(block_step), initial, (x_blocks, decay_blocks, write_blocks, read_blocks))
    return outputs.reshape(total, head_count, head_width)

def add_block(running, pair):
    part_sum = jnp.dot(pair[0].T, pair[1], preferred_element_type=jnp.float32)
    rounded = lax.optimization_barrier(part_sum.astype(jnp.bfloat16))
    return (running + rounded.astype(jnp.float32), None)

def reference(packed_input, block_exponent, gate_input, state_write, state_read, log_decay, skip_weight, norm_gain, out_weight, out_cotangent):
    x_values = dequantize(packed_input, block_exponent)
    total, width = x_values.shape
    head_count = log_decay.shape[0]
    x_heads = x_values.astype(jnp.float32).reshape(total, head_count, width // head_count)
    write_rows = state_write.astype(jnp.float32)
    read_rows = state_read.astype(jnp.float32)
    core, pullback = jax.vjp(scan_states, x_heads, log_decay, write_rows, read_rows)
    y_full = (core + skip_weight[None, :, None] * x_heads).reshape(total, width)
    gate = gate_input.astype(jnp.float32)
    sigma = jax.nn.sigmoid(gate)
    active = gate * sigma
    mixed = y_full * active
    scale_row = lax.rsqrt(lax.optimization_barrier(jnp.mean(mixed * mixed, axis=1, keepdims=True)) + 1e-05)
    normed = (mixed * scale_row * norm_gain).astype(jnp.bfloat16)
    grad_v = jnp.dot(out_cotangent, out_weight.T, preferred_element_type=jnp.float32)
    model_width = out_weight.shape[1]
    normed_blocks = normed.reshape(-1, TOK_DEV, width)
    cot_blocks = out_cotangent.reshape(-1, TOK_DEV, model_width)
    grad_out_weight, _ = lax.scan(add_block, jnp.zeros((width, model_width), jnp.float32), (normed_blocks, cot_blocks))
    scaled = grad_v * norm_gain
    grad_gain = lax.optimization_barrier(jnp.sum(grad_v * mixed * scale_row, axis=0))
    inner = lax.optimization_barrier(jnp.sum(scaled * mixed, axis=1, keepdims=True))
    grad_mixed = scale_row * scaled - mixed * (scale_row * scale_row * scale_row) * inner / width
    grad_gate = (grad_mixed * y_full * sigma * (1.0 + gate * (1.0 - sigma))).astype(jnp.bfloat16)
    grad_y = (grad_mixed * active).reshape(total, head_count, width // head_count)
    grad_skip = lax.optimization_barrier(jnp.sum(grad_y * x_heads, axis=(0, 2)))
    grad_core, grad_decay, grad_write, grad_read = pullback(grad_y)
    grad_input = (grad_core + skip_weight[None, :, None] * grad_y).reshape(total, width).astype(jnp.bfloat16)
    return (grad_input, grad_gate, grad_write, grad_read, grad_decay, grad_skip, grad_gain, grad_out_weight)
```

```python
import jax
import jax.numpy as jnp
from jax import lax
from jax.experimental import pallas as pl
from jax.experimental.pallas import tpu as pltpu
from jax.sharding import PartitionSpec as P

PRECISE = lax.Precision.HIGHEST
F32 = jnp.float32
BF16 = jnp.bfloat16
LANES = 128
CHUNK = 128
VMEM_LIMIT = 48 * 1024 * 1024

FACTOR, SEG, SEG_EXP, TO_CHUNK_END, FROM_START, TO_END = 0, 1, 3, 5, 7, 9
COLUMN_COUNT = 16


def dot(a, b, contract):
    return lax.dot_general(a, b, ((contract[:1], contract[1:]), ((), ())), preferred_element_type=F32)


def spread_pair(columns, at, rows):
    lane = lax.broadcasted_iota(jnp.int32, (rows, LANES), 1)
    return jnp.where(lane < LANES // 2, columns[:, at : at + 1], columns[:, at + 1 : at + 2])


def chunk_decay(columns, seg_rows, head, rows):
    token = lax.broadcasted_iota(jnp.int32, (rows, rows), 0)
    source = lax.broadcasted_iota(jnp.int32, (rows, rows), 1)
    spread = columns[:, SEG + head : SEG + head + 1] - seg_rows[head : head + 1, :]
    return jnp.exp(jnp.where(token >= source, spread, -1e30))


def unpack_kernel(packed_ref, col_ref, write_t_ref, x_ref, state_ref):
    words = packed_ref[...]
    groups = words.shape[0]
    length = groups * 8
    wide = jnp.broadcast_to(words[:, None, :], (groups, 8, LANES))
    shifts = 4 * lax.broadcasted_iota(jnp.int32, (groups, 8, LANES), 1)
    fields = jnp.bitwise_and(jnp.right_shift(wide, shifts), 15) - 8
    columns = col_ref[0]
    x = fields.astype(F32).reshape(length, LANES) * columns[:, FACTOR : FACTOR + 1]
    x_ref[...] = x.astype(BF16)
    weighted = (x * spread_pair(columns, TO_END, length)).astype(BF16)
    state_ref[...] = dot(write_t_ref[...], weighted, (1, 0)).astype(BF16)


def local_kernel(x_ref, col_ref, seg_ref, row_ref, cross_ref, write_t_ref, read_ref, y_ref):
    length = x_ref.shape[0]
    chunk = min(CHUNK, length)
    lane = lax.broadcasted_iota(jnp.int32, (chunk, LANES), 1)
    state = None
    for c in range(length // chunk):
        part = pl.ds(c * chunk, chunk)
        columns = col_ref[0, part, :]
        seg_rows = seg_ref[0, :, part]
        x = x_ref[part, :]
        cross = cross_ref[c]
        halves = []
        for head in range(2):
            mixing = (chunk_decay(columns, seg_rows, head, chunk) * cross).astype(BF16)
            halves.append(dot(mixing, x, (1, 0)))
        y = jnp.where(lane < LANES // 2, halves[0], halves[1])
        if state is not None:
            y = y + spread_pair(columns, SEG_EXP, chunk) * dot(
                read_ref[part, :], state.astype(BF16), (1, 0)
            )
        y_ref[part, :] = y
        weighted = (x.astype(F32) * spread_pair(columns, TO_CHUNK_END, chunk)).astype(BF16)
        added = dot(write_t_ref[:, part], weighted, (1, 0))
        state = added if state is None else state * row_ref[0, c + 3 : c + 4, :] + added


def weigh_pieces(piece_ref, weight_ref):
    total = None
    for k in range(piece_ref.shape[0]):
        term = piece_ref[k].astype(F32) * weight_ref[0, k : k + 1, :]
        total = term if total is None else total + term
    return total


def mix_kernel(
    y_local_ref, x_ref, col_ref, row_ref, read_ref, piece_ref, weight_ref, gate_ref, grad_v_ref,
    y_ref, state_ref, square_ref, inner_ref,
):
    length = x_ref.shape[0]
    state = weigh_pieces(piece_ref, weight_ref)
    state_ref[...] = state
    carried = dot(read_ref[...], state.astype(BF16), (1, 0))
    y = (
        y_local_ref[...]
        + spread_pair(col_ref[0], FROM_START, length) * carried
        + row_ref[0, 0:1, :] * x_ref[...].astype(F32)
    )
    y_ref[...] = y
    gate = gate_ref[...].astype(F32)
    mixed = y * gate * jax.nn.sigmoid(gate)
    square = mixed * mixed
    inner = grad_v_ref[...] * row_ref[0, 1:2, :] * mixed

    @pl.when(pl.program_id(0) == 0)
    def _():
        square_ref[...] = square
        inner_ref[...] = inner

    @pl.when(pl.program_id(0) > 0)
    def _():
        square_ref[...] += square
        inner_ref[...] += inner


def gate_kernel(
    y_ref, x_ref, col_ref, row_ref, read_t_ref, gate_ref, grad_v_ref, scale_ref,
    normed_ref, grad_gate_ref, grad_y_ref, sums_ref, cot_ref,
):
    length = x_ref.shape[0]
    scale = scale_ref[:, 0:1]
    pull = scale_ref[:, 1:2]
    gain = row_ref[0, 1:2, :]
    y = y_ref[...]
    gate = gate_ref[...].astype(F32)
    sigma = jax.nn.sigmoid(gate)
    active = gate * sigma
    mixed = y * active
    mixed_scaled = mixed * scale
    normed_ref[...] = (mixed_scaled * gain).astype(BF16)
    grad_v = grad_v_ref[...]
    grad_mixed = scale * grad_v * gain - mixed * pull
    grad_gate_ref[...] = (grad_mixed * y * sigma * (1.0 + gate * (1.0 - sigma))).astype(BF16)
    grad_y = grad_mixed * active
    grad_y_ref[...] = grad_y.astype(BF16)
    gain_sum = jnp.sum(grad_v * mixed_scaled, axis=0, keepdims=True)
    skip_sum = jnp.sum(grad_y * x_ref[...].astype(F32), axis=0, keepdims=True)
    sums_ref[0, 0:1, :] = gain_sum
    sums_ref[0, 1:2, :] = skip_sum
    weighted = (grad_y * spread_pair(col_ref[0], FROM_START, length)).astype(BF16)
    cot_ref[...] = dot(read_t_ref[...], weighted, (1, 0)).astype(BF16)


def back_kernel(
    x_ref, grad_y_ref, y_ref, col_ref, seg_ref, row_ref, cross_ref, write_ref, read_ref,
    write_t_ref, read_t_ref, state_ref, piece_ref, weight_ref,
    grad_x_ref, grad_map_ref, diff_ref, const_ref, summed_ref,
):
    pair = pl.program_id(0)
    length = x_ref.shape[0]
    chunk = min(CHUNK, length)
    chunks = length // chunk
    lane = lax.broadcasted_iota(jnp.int32, (chunk, LANES), 1)
    is_first = lane < LANES // 2
    states = [state_ref[...]]
    weighted_x = []
    for c in range(chunks):
        part = pl.ds(c * chunk, chunk)
        to_end = spread_pair(col_ref[0, part, :], TO_CHUNK_END, chunk)
        weighted_x.append((x_ref[part, :].astype(F32) * to_end).astype(BF16))
        if c < chunks - 1:
            states.append(
                states[-1] * row_ref[0, c + 3 : c + 4, :]
                + dot(write_t_ref[:, part], weighted_x[-1], (1, 0))
            )

    @pl.when(pair == 0)
    def _():
        grad_map_ref[...] = jnp.zeros_like(grad_map_ref)
        summed_ref[...] = jnp.zeros_like(summed_ref)

    skip = row_ref[0, 0:1, :]
    carry = weigh_pieces(piece_ref, weight_ref)
    for c in reversed(range(chunks)):
        part = pl.ds(c * chunk, chunk)
        columns = col_ref[0, part, :]
        seg_rows = seg_ref[0, :, part]
        x16 = x_ref[part, :]
        x = x16.astype(F32)
        g16 = grad_y_ref[part, :]
        g = g16.astype(F32)
        cross = cross_ref[c]
        state = states[c]
        chunk_exp = row_ref[0, c + 3 : c + 4, :]
        carry16 = carry.astype(BF16)
        leaving = spread_pair(columns, TO_CHUNK_END, chunk) * dot(write_ref[part, :], carry16, (1, 0))
        halves = []
        summed = None
        for head in range(2):
            decay = chunk_decay(columns, seg_rows, head, chunk)
            mixing = (decay * cross).astype(BF16)
            halves.append(dot(mixing, g16, (0, 0)))
            own = is_first if head == 0 else jnp.logical_not(is_first)
            pair_dot = dot(jnp.where(own, g, 0.0).astype(BF16), x16, (1, 1)) * decay
            summed = pair_dot if summed is None else summed + pair_dot
        summed_ref[c] += summed
        grad_x = jnp.where(is_first, halves[0], halves[1]) + leaving
        grad_x_ref[part, :] = (skip * g + grad_x).astype(BF16)
        diff = g * (y_ref[part, :] - skip * x) - x * grad_x
        diff_ref[0, part, 0:1] = jnp.sum(jnp.where(is_first, diff, 0.0), axis=1, keepdims=True)
        diff_ref[0, part, 1:2] = jnp.sum(jnp.where(is_first, 0.0, diff), axis=1, keepdims=True)
        const_ref[0, c : c + 1, :] = jnp.sum(x * leaving, axis=0, keepdims=True) + chunk_exp * jnp.sum(
            carry * state, axis=0, keepdims=True
        )
        weighted_g = (g * spread_pair(columns, SEG_EXP, chunk)).astype(BF16)
        grad_map_ref[part, :LANES] += dot(weighted_x[c], carry16, (1, 1))
        grad_map_ref[part, LANES:] += dot(weighted_g, state.astype(BF16), (1, 1))
        carry = carry * chunk_exp + dot(read_t_ref[:, part], weighted_g, (1, 0))

    @pl.when(pair == pl.num_programs(0) - 1)
    def _():
        for c in range(chunks):
            part = pl.ds(c * chunk, chunk)
            summed = summed_ref[c].astype(BF16)
            grad_map_ref[part, :LANES] += dot(summed, read_ref[part, :], (0, 0))
            grad_map_ref[part, LANES:] += dot(summed, write_ref[part, :], (1, 0))


def on_device(
    packed_input,
    block_exponent,
    gate_input,
    state_write,
    state_read,
    log_decay,
    skip_weight,
    norm_gain,
    out_weight,
    out_cotangent,
):
    head_count, length = log_decay.shape
    width = packed_input.shape[1]
    states = state_write.shape[1]
    head_width = width // head_count
    pairs = width // LANES
    per_pair = head_count // pairs
    chunk = min(CHUNK, length)
    chunks = length // chunk
    total_width = width * lax.axis_size("tp")
    position = lax.axis_index("seq")
    sequence = lax.axis_size("seq")

    cot_full = lax.all_gather(out_cotangent, "tp", axis=1, tiled=True)

    order = jnp.arange(chunk)
    upper = (order[:, None] <= order[None, :]).astype(F32)
    decay_chunks = log_decay.reshape(head_count * chunks, chunk)
    seg = jnp.dot(decay_chunks, upper, precision=PRECISE).reshape(head_count, chunks, chunk)
    chunk_total = seg[:, :, -1]
    chunk_running = jnp.cumsum(chunk_total, axis=1)
    decay_total = chunk_running[:, -1]
    decay_sum = (seg + (chunk_running - chunk_total)[:, :, None]).reshape(head_count, length)
    to_chunk_end = jnp.exp(chunk_total[:, :, None] - seg).reshape(head_count, length)
    seg = seg.reshape(head_count, length)
    to_end = jnp.exp(decay_total[:, None] - decay_sum)
    factor = jnp.exp2(block_exponent.astype(F32))

    def paired(a):
        return a.reshape(pairs, per_pair, length)

    stacked = jnp.concatenate(
        [
            factor[:, None, :],
            paired(seg),
            paired(jnp.exp(seg)),
            paired(to_chunk_end),
            paired(jnp.exp(decay_sum)),
            paired(to_end),
            jnp.zeros((pairs, COLUMN_COUNT - 1 - 5 * per_pair, length), F32),
        ],
        axis=1,
    )
    columns = stacked.transpose(0, 2, 1)
    seg_rows = paired(seg)

    def widen(a):
        return jnp.repeat(a, head_width, axis=-1)

    rows = jnp.stack(
        [widen(skip_weight), norm_gain, jnp.zeros_like(norm_gain)]
        + [widen(jnp.exp(chunk_total[:, c])) for c in range(chunks)],
        axis=0,
    )
    row_count = rows.shape[0]
    rows = rows.reshape(row_count, pairs, LANES).transpose(1, 0, 2)

    totals = lax.all_gather(decay_total[None], "seq", axis=0, tiled=True)
    running = jnp.cumsum(totals, axis=0)
    running_here = lax.dynamic_index_in_dim(running, position, 0, keepdims=False)
    before_here = running_here - decay_total
    sources = jnp.arange(sequence)
    is_earlier = (sources < position)[:, None]
    is_later = (sources > position)[:, None]
    early = jnp.where(
        is_earlier, jnp.exp(jnp.where(is_earlier, before_here[None] - running, 0.0)), 0.0
    )
    late = jnp.where(
        is_later, jnp.exp(jnp.where(is_later, running - totals - running_here[None], 0.0)), 0.0
    )

    def by_pair(weights):
        return widen(weights).reshape(sequence, pairs, LANES).transpose(1, 0, 2)

    early, late = by_pair(early), by_pair(late)

    write_t, read_t = state_write.T, state_read.T
    cross = lax.dot_general(
        state_read.reshape(chunks, chunk, states),
        state_write.reshape(chunks, chunk, states),
        (((2,), (2,)), ((0,), (0,))),
        preferred_element_type=F32,
    )

    wide_spec = pl.BlockSpec((length, LANES), lambda i: (0, i))
    col_spec = pl.BlockSpec((1, length, COLUMN_COUNT), lambda i: (i, 0, 0))
    seg_spec = pl.BlockSpec((1, per_pair, length), lambda i: (i, 0, 0))
    row_spec = pl.BlockSpec((1, row_count, LANES), lambda i: (i, 0, 0))
    cross_spec = pl.BlockSpec((chunks, chunk, chunk), lambda i: (0, 0, 0))
    map_spec = pl.BlockSpec((length, states), lambda i: (0, 0))
    map_t_spec = pl.BlockSpec((states, length), lambda i: (0, 0))
    state_spec = pl.BlockSpec((states, LANES), lambda i: (0, i))
    piece_spec = pl.BlockSpec((sequence, states, LANES), lambda i: (0, 0, i))
    weight_spec = pl.BlockSpec((1, sequence, LANES), lambda i: (i, 0, 0))
    shape = jax.ShapeDtypeStruct

    def call(kernel, in_specs, out_specs, out_shape, micros):
        return pl.pallas_call(
            kernel,
            grid=(pairs,),
            in_specs=in_specs,
            out_specs=out_specs,
            out_shape=out_shape,
            compiler_params=pltpu.CompilerParams(
                dimension_semantics=("arbitrary",), vmem_limit_bytes=VMEM_LIMIT
            ),
            cost_estimate=pl.CostEstimate(
                flops=int(micros * 9e8), bytes_accessed=int(micros * 1e5), transcendentals=0
            ),
        )

    x, local_state = call(
        unpack_kernel,
        [pl.BlockSpec((length // 8, LANES), lambda i: (0, i)), col_spec, map_t_spec],
        [wide_spec, state_spec],
        [shape((length, width), BF16), shape((states, width), BF16)],
        4,
    )(packed_input, columns, write_t)
    state_pieces = lax.all_gather(local_state[None], "seq", axis=0, tiled=True)

    y_local = call(
        local_kernel,
        [wide_spec, col_spec, seg_spec, row_spec, cross_spec, map_t_spec, map_spec],
        wide_spec,
        shape((length, width), F32),
        10,
    )(x, columns, seg_rows, rows, cross, write_t, state_read)
    grad_v = lax.dot_general(
        cot_full, out_weight, (((1,), (1,)), ((), ())), preferred_element_type=F32
    )

    y_full, state_in, square, inner = call(
        mix_kernel,
        [
            wide_spec, wide_spec, col_spec, row_spec, map_spec, piece_spec, weight_spec,
            wide_spec, wide_spec,
        ],
        [wide_spec, state_spec, map_spec, map_spec],
        [
            shape((length, width), F32),
            shape((states, width), F32),
            shape((length, LANES), F32),
            shape((length, LANES), F32),
        ],
        6,
    )(y_local, x, columns, rows, state_read, state_pieces, early, gate_input, grad_v)
    token_sums = lax.psum(jnp.stack([jnp.sum(square, axis=1), jnp.sum(inner, axis=1)]), "tp")
    scale = lax.rsqrt(token_sums[0] / total_width + 1e-05)
    pull = scale * scale * scale * token_sums[1] / total_width
    scales = jnp.stack([scale, pull], axis=1)

    normed, grad_gate, grad_y, sums, local_cot = call(
        gate_kernel,
        [
            wide_spec, wide_spec, col_spec, row_spec, map_t_spec, wide_spec, wide_spec,
            pl.BlockSpec((length, 2), lambda i: (0, 0)),
        ],
        [
            wide_spec, wide_spec, wide_spec,
            pl.BlockSpec((1, 2, LANES), lambda i: (i, 0, 0)),
            state_spec,
        ],
        [
            shape((length, width), BF16),
            shape((length, width), BF16),
            shape((length, width), BF16),
            shape((pairs, 2, LANES), F32),
            shape((states, width), BF16),
        ],
        6,
    )(y_full, x, columns, rows, read_t, gate_input, grad_v, scales)
    cot_pieces = lax.all_gather(local_cot[None], "seq", axis=0, tiled=True)
    product = lax.dot_general(
        cot_full, normed, (((0,), (0,)), ((), ())), preferred_element_type=F32
    ).astype(BF16)
    product = product.reshape(sequence, -1, width)
    arrived = [lax.dynamic_index_in_dim(product, position, 0, keepdims=False)]
    for step in range(1, sequence):
        block = lax.dynamic_index_in_dim(product, (position + step) % sequence, 0, keepdims=False)
        route = [(source, (source + step) % sequence) for source in range(sequence)]
        arrived.append(lax.ppermute(block, "seq", route))
    grad_out_weight = sum(block.astype(F32) for block in arrived).T
    gain_part = sums[:, 0, :].reshape(width)
    skip_part = jnp.sum(sums[:, 1, :].reshape(head_count, head_width), axis=1)
    grad_gain, grad_skip = lax.psum((gain_part, skip_part), "seq")

    grad_input, grad_map, diff, const, _ = call(
        back_kernel,
        [
            wide_spec, wide_spec, wide_spec, col_spec, seg_spec, row_spec, cross_spec,
            map_spec, map_spec, map_t_spec, map_t_spec, state_spec, piece_spec, weight_spec,
        ],
        [
            wide_spec,
            pl.BlockSpec((length, 2 * states), lambda i: (0, 0)),
            pl.BlockSpec((1, length, per_pair), lambda i: (i, 0, 0)),
            pl.BlockSpec((1, chunks, LANES), lambda i: (i, 0, 0)),
            cross_spec,
        ],
        [
            shape((length, width), BF16),
            shape((length, 2 * states), F32),
            shape((pairs, length, per_pair), F32),
            shape((pairs, chunks, LANES), F32),
            shape((chunks, chunk, chunk), F32),
        ],
        20,
    )(
        x, grad_y, y_full, columns, seg_rows, rows, cross, state_write, state_read,
        write_t, read_t, state_in, cot_pieces, late,
    )
    grad_map = lax.psum(grad_map, "tp")
    grad_write, grad_read = grad_map[:, :states], grad_map[:, states:]
    diff_rows = diff.transpose(0, 2, 1).reshape(head_count * chunks, chunk)
    suffix = jnp.dot(diff_rows, upper.T, precision=PRECISE).reshape(head_count, chunks, chunk)
    const = jnp.sum(const.reshape(pairs, chunks, per_pair, head_width), axis=3)
    const = const.transpose(0, 2, 1).reshape(head_count, chunks)
    grad_decay = (suffix + const[:, :, None]).reshape(head_count, length)
    return (
        grad_input,
        grad_gate,
        grad_write,
        grad_read,
        grad_decay,
        grad_skip,
        grad_gain,
        grad_out_weight,
    )


def solution(mesh):
    placed = (
        P("seq", "tp"),
        P("tp", "seq"),
        P("seq", "tp"),
        P("seq", None),
        P("seq", None),
        P("tp", "seq"),
        P("tp"),
        P("tp"),
        P("tp", None),
        P("seq", "tp"),
    )
    return jax.shard_map(
        on_device,
        mesh=mesh,
        in_specs=placed,
        out_specs=(
            P("seq", "tp"),
            P("seq", "tp"),
            P("seq", None),
            P("seq", None),
            P("tp", "seq"),
            P("tp"),
            P("tp"),
            P("tp", "seq"),
        ),
        check_vma=False,
    )
```
